16 devices in a mesh: dp: 2 (over y, z), tp: 8 (over x, core).
Axes of the slice: x: 4, y: 2, z: 1, core: 2. Of those that a mesh axis runs over, the one named last changes fastest.
The devices are a block of a 4x4x8 slice.
Arguments:
- hidden: bfloat16 [16, 1024, 2304], P('dp', 'tp'), parts along dimension 0
- ln1_gain: float32 [2304], replicated
- ln1_bias: float32 [2304], replicated
- w_qkv: bfloat16 [2304, 3, 24, 96], P(None, None, 'tp')
- b_qkv: bfloat16 [3, 24, 96], P(None, 'tp')
- w_out: bfloat16 [24, 96, 2304], P('tp')
- b_out: bfloat16 [2304], replicated
- ln2_gain: float32 [2304], replicated
- ln2_bias: float32 [2304], replicated
- w_up: bfloat16 [2304, 9216], P(None, 'tp')
- b_up: bfloat16 [9216], P('tp')
- w_down: bfloat16 [9216, 2304], P('tp')
- b_down: bfloat16 [2304], replicated
Outputs:
- output: bfloat16 [16, 1024, 2304], P('dp', 'tp'), parts along dimension 0
There are 2 independent parts. The reference program is written for one: setup_inputs(seed, part) draws one part's arguments, and reference() takes and returns one part's arrays. A program takes and returns all parts, laid end to end along the dimension named above; an argument that names none is the same for every part.
All inputs are finite; a program needn't handle non-finite values.
Results may differ from the reference program's by a relative error of at most 0.0105948.
Values are sent between devices in bfloat16 or wider.
A program may use at most 768 MiB of HBM per device.

```python
import math
import jax
import jax.numpy as jnp
from jax import lax

N_BATCH = 8
SEQ_LEN = 1024
D_MODEL = 2304
N_HEADS = 24

HEAD_DIM = D_MODEL // N_HEADS
FF_DIM = 4 * D_MODEL
LN_EPS = 1e-5


def layer_norm(inputs, gain_vec, shift_vec):
    as_f32 = inputs.astype(jnp.float32)
    row_mean = jnp.mean(as_f32, axis=-1, keepdims=True)
    centered = as_f32 - row_mean
    variance = jnp.mean(centered * centered, axis=-1, keepdims=True)
    return (centered * lax.rsqrt(variance + LN_EPS) * gain_vec + shift_vec).astype(jnp.bfloat16)


def setup_inputs(seed: int = 0, part: int = 0) -> dict:
    root_key = jax.random.key(seed)
    sub_keys = jax.random.split(root_key, 13)
    qk_gain = (0.5 * math.log(SEQ_LEN)) ** 0.25
    col_gain = jnp.array([qk_gain, qk_gain, 1.0], jnp.float32).reshape(1, 3, 1, 1)
    hidden = jax.random.normal(jax.random.fold_in(sub_keys[0], part), (N_BATCH, SEQ_LEN, D_MODEL), jnp.float32)
    w_qkv = jax.random.normal(sub_keys[3], (D_MODEL, 3, N_HEADS, HEAD_DIM), jnp.float32) * col_gain * D_MODEL ** -0.5
    return {
        "hidden": hidden.astype(jnp.bfloat16),
        "ln1_gain": 1.0 + 0.3 * jax.random.normal(sub_keys[1], (D_MODEL,), jnp.float32),
        "ln1_bias": 0.3 * jax.random.normal(sub_keys[2], (D_MODEL,), jnp.float32),
        "w_qkv": w_qkv.astype(jnp.bfloat16),
        "b_qkv": (0.5 * jax.random.normal(sub_keys[4], (3, N_HEADS, HEAD_DIM), jnp.float32)).astype(jnp.bfloat16),
        "w_out": (jax.random.normal(sub_keys[5], (N_HEADS, HEAD_DIM, D_MODEL), jnp.float32) * D_MODEL ** -0.5).astype(jnp.bfloat16),
        "b_out": (0.3 * jax.random.normal(sub_keys[6], (D_MODEL,), jnp.float32)).astype(jnp.bfloat16),
        "ln2_gain": 1.0 + 0.3 * jax.random.normal(sub_keys[7], (D_MODEL,), jnp.float32),
        "ln2_bias": 0.3 * jax.random.normal(sub_keys[8], (D_MODEL,), jnp.float32),
        "w_up": (jax.random.normal(sub_keys[9], (D_MODEL, FF_DIM), jnp.float32) * D_MODEL ** -0.5).astype(jnp.bfloat16),
        "b_up": (0.5 * jax.random.normal(sub_keys[10], (FF_DIM,), jnp.float32)).astype(jnp.bfloat16),
        "w_down": (jax.random.normal(sub_keys[11], (FF_DIM, D_MODEL), jnp.float32) * FF_DIM ** -0.5).astype(jnp.bfloat16),
        "b_down": (0.3 * jax.random.normal(sub_keys[12], (D_MODEL,), jnp.float32)).astype(jnp.bfloat16),
    }


def reference(hidden, ln1_gain, ln1_bias, w_qkv, b_qkv, w_out, b_out, ln2_gain, ln2_bias, w_up, b_up, w_down, b_down):
    normed = layer_norm(hidden, ln1_gain, ln1_bias).reshape(N_BATCH * SEQ_LEN, D_MODEL)
    qkv_acc = jnp.dot(normed, w_qkv.reshape(D_MODEL, 3 * D_MODEL), preferred_element_type=jnp.float32)
    qkv_all = (qkv_acc + b_qkv.reshape(3 * D_MODEL).astype(jnp.float32)).astype(jnp.bfloat16)
    head_major = jnp.transpose(qkv_all.reshape(N_BATCH, SEQ_LEN, 3, N_HEADS, HEAD_DIM), (2, 3, 0, 1, 4))
    positions = jnp.arange(SEQ_LEN)
    causal = positions[:, None] >= positions[None, :]

    def one_head(operands):
        queries, keys_all, values = operands
        logits = jnp.einsum("bqd,bkd->bqk", queries.astype(jnp.float32), keys_all.astype(jnp.float32)) * HEAD_DIM ** -0.5
        logits = jnp.where(causal, logits, -1e30)
        row_max = jnp.max(logits, axis=-1, keepdims=True)
        exp_vals = jnp.exp(logits - row_max)
        weights_bf = (exp_vals / jnp.sum(exp_vals, axis=-1, keepdims=True)).astype(jnp.bfloat16)
        return jnp.einsum("bqk,bkd->bqd", weights_bf.astype(jnp.float32), values.astype(jnp.float32)).astype(jnp.bfloat16)

    context = lax.map(one_head, (head_major[0], head_major[1], head_major[2]))
    attn_sum = jnp.einsum("hbsd,hde->bse", context.astype(jnp.float32), w_out.astype(jnp.float32))
    resid_mid = (hidden.astype(jnp.float32) + (attn_sum + b_out.astype(jnp.float32))).astype(jnp.bfloat16)
    normed_mid = layer_norm(resid_mid, ln2_gain, ln2_bias).reshape(N_BATCH * SEQ_LEN, D_MODEL)
    up_proj = jnp.dot(normed_mid, w_up, preferred_element_type=jnp.float32) + b_up.astype(jnp.float32)
    gelu_out = jax.nn.gelu(up_proj, approximate=True).astype(jnp.bfloat16)
    down_sum = jnp.dot(gelu_out, w_down, preferred_element_type=jnp.float32) + b_down.astype(jnp.float32)
    return (resid_mid.astype(jnp.float32) + down_sum.reshape(N_BATCH, SEQ_LEN, D_MODEL)).astype(jnp.bfloat16)
```

```python
import functools

import jax
import jax.numpy as jnp
from jax import lax
from jax.experimental import pallas as pl
from jax.experimental.pallas import tpu as pltpu
from jax.sharding import PartitionSpec as P

LN_EPS = 1e-5
BF16, F32 = jnp.bfloat16, jnp.float32
QUERY_BLOCK = 256


def layer_norm(inputs, gain_vec, shift_vec):
    as_f32 = inputs.astype(F32)
    row_mean = jnp.mean(as_f32, axis=-1, keepdims=True)
    centered = as_f32 - row_mean
    variance = jnp.mean(centered * centered, axis=-1, keepdims=True)
    return (centered * lax.rsqrt(variance + LN_EPS) * gain_vec + shift_vec).astype(BF16)


def attention_kernel(n_blocks, scale, place_ref, *refs):
    qkv_refs, ctx_ref = refs[:n_blocks], refs[n_blocks]
    q_all, k_all, v_all, c_all = refs[n_blocks + 1:]
    blk = qkv_refs[0].shape[-1]
    for m in range(n_blocks):
        where = pl.ds(pl.multiple_of(place_ref[m] * blk, blk), blk)
        q_all[:, where] = qkv_refs[m][0, 0, 0]
        k_all[:, where] = qkv_refs[m][0, 1, 0]
        v_all[:, where] = qkv_refs[m][0, 2, 0]
    seq_len = n_blocks * blk
    keys = k_all[...].T
    log2_scale = scale * 1.4426950408889634
    for start in range(0, seq_len, QUERY_BLOCK):
        stop = start + QUERY_BLOCK
        logits = jnp.dot(keys[:stop], q_all[:, start:stop], preferred_element_type=F32)
        key_pos = lax.broadcasted_iota(jnp.int32, (QUERY_BLOCK, QUERY_BLOCK), 0)
        query_pos = lax.broadcasted_iota(jnp.int32, (QUERY_BLOCK, QUERY_BLOCK), 1)
        diag = jnp.where(key_pos <= query_pos, logits[start:], -1e30)
        logits = jnp.concatenate([logits[:start], diag], axis=0) if start else diag
        row_max = jnp.max(logits, axis=0, keepdims=True)
        exp_vals = jnp.exp2((logits - row_max) * log2_scale)
        weights = (exp_vals * (1.0 / jnp.sum(exp_vals, axis=0, keepdims=True))).astype(BF16)
        c_all[:, start:stop] = jnp.dot(v_all[:, :stop], weights, preferred_element_type=F32).astype(BF16)
    for m in range(n_blocks):
        where = pl.ds(pl.multiple_of(place_ref[m] * blk, blk), blk)
        ctx_ref[m, 0] = c_all[:, where]


def attention(place, qkv_blocks):
    n_blocks = len(qkv_blocks)
    seqs, _, heads, dim, blk = qkv_blocks[0].shape
    total = n_blocks * blk
    pairs = total * total // 2
    return pl.pallas_call(
        functools.partial(attention_kernel, n_blocks, dim ** -0.5),
        grid_spec=pltpu.PrefetchScalarGridSpec(
            num_scalar_prefetch=1,
            grid=(seqs, heads),
            in_specs=[pl.BlockSpec((1, 3, 1, dim, blk), lambda b, j, place: (b, 0, j, 0, 0))] * n_blocks,
            out_specs=pl.BlockSpec((n_blocks, 1, dim, blk), lambda b, j, place: (0, b, j, 0)),
            scratch_shapes=[pltpu.VMEM((dim, total), BF16)] * 4,
        ),
        out_shape=jax.ShapeDtypeStruct((n_blocks, seqs, heads * dim, blk), BF16),
        compiler_params=pltpu.CompilerParams(dimension_semantics=("parallel", "parallel"), vmem_limit_bytes=32 * 1024 * 1024),
        cost_estimate=pl.CostEstimate(
            flops=seqs * heads * pairs * dim * 4, bytes_accessed=seqs * heads * total * dim * 8, transcendentals=seqs * heads * pairs
        ),
        name="attention",
    )(place, *qkv_blocks)


def solution(mesh):
    group = mesh.shape["tp"]
    SIB, NEAR, FAR = 1, 2, group - 2
    ACROSS = NEAR ^ FAR

    def swap(value, mask):
        return lax.ppermute(value, "tp", [(i, i ^ mask) for i in range(group)])

    def device_body(hidden, ln1_gain, ln1_bias, w_qkv, b_qkv, w_out, b_out, ln2_gain, ln2_bias, w_up, b_up, w_down, b_down):
        me = lax.axis_index("tp")
        n_seq, _, width = hidden.shape
        half = n_seq // 2
        side = me // (group // 2)
        x_own = lax.dynamic_slice_in_dim(hidden, side * half, half, 0)
        x_oth = lax.dynamic_slice_in_dim(hidden, (1 - side) * half, half, 0)

        rows = {}
        h_oth = layer_norm(x_oth, ln1_gain, ln1_bias)
        rows[0] = layer_norm(x_own, ln1_gain, ln1_bias)
        rows[FAR] = swap(h_oth, FAR)
        rows[NEAR] = swap(rows[0], NEAR)
        rows[ACROSS] = swap(rows[FAR], NEAR)
        for m in (0, FAR, NEAR, ACROSS):
            rows[m ^ SIB] = swap(rows[m], SIB)

        bq_far = swap(b_qkv, FAR)
        wq_far = swap(w_qkv, FAR)

        place = jnp.arange(group, dtype=jnp.int32) ^ me

        def heads_ctx(weights, bias):
            shift = bias.astype(F32)[None, :, :, :, None]
            blocks = []
            for m in range(group):
                acc = jnp.einsum("bsd,dthe->bthes", rows[m], weights, preferred_element_type=F32)
                blocks.append((acc + shift).astype(BF16))
            return attention(place, blocks)

        def to_owners(ctx):
            got = {0: ctx[0]}
            got[SIB] = swap(ctx[SIB], SIB)
            for m in (NEAR, FAR, ACROSS):
                both = swap(ctx[m:m + 2], m)
                got[m] = both[0]
                got[m ^ SIB] = swap(both[1], SIB)
            near_side = jnp.concatenate([got[m] for m in (0, NEAR, SIB, NEAR ^ SIB)], axis=1)
            far_side = jnp.concatenate([got[m] for m in (FAR, ACROSS, FAR ^ SIB, ACROSS ^ SIB)], axis=1)
            return near_side, far_side

        ctx_a = heads_ctx(w_qkv, b_qkv)
        a_own, a_oth = to_owners(ctx_a)
        ctx_b = heads_ctx(wq_far, bq_far)
        b_own, b_oth = to_owners(ctx_b)

        wo = {0: w_out.reshape(-1, width)}
        wo[FAR] = swap(wo[0], FAR)
        wo[NEAR] = swap(wo[0], NEAR)
        wo[ACROSS] = swap(wo[NEAR], FAR)
        for m in (0, NEAR, FAR, ACROSS):
            wo[m ^ SIB] = swap(wo[m], SIB)
        wo_near = jnp.concatenate([wo[m] for m in (0, NEAR, SIB, NEAR ^ SIB)], axis=0)
        wo_far = jnp.concatenate([wo[m] for m in (FAR, ACROSS, FAR ^ SIB, ACROSS ^ SIB)], axis=0)

        def project(ctx, weights):
            return jnp.einsum("bcs,ce->bse", ctx, weights, preferred_element_type=F32)

        def mid(x, attn):
            x1 = (x.astype(F32) + (attn + b_out.astype(F32))).astype(BF16)
            return x1, layer_norm(x1, ln2_gain, ln2_bias)

        x1_own, h2_own = mid(x_own, project(a_own, wo_near) + project(b_own, wo_far))
        x1_oth, h2_oth = mid(x_oth, project(a_oth, wo_far) + project(b_oth, wo_near))

        n_parts = 3
        part_up, part_dn = w_up.shape[1] // n_parts, width // n_parts
        ups = [(w_up, b_up)]
        ups.append((swap(w_up, SIB), swap(b_up, SIB)))
        bu_near = swap(b_up, NEAR)
        bu_near_sib = swap(bu_near, SIB)
        near_parts, near_sib_parts = [], []
        for i in range(n_parts):
            cols = slice(i * part_up, (i + 1) * part_up)
            got = swap(w_up[:, cols], NEAR)
            near_parts.append((got, bu_near[cols]))
            near_sib_parts.append((swap(got, SIB), bu_near_sib[cols]))
        wd_sib = swap(w_down, SIB)
        downs = []
        for i in range(n_parts):
            cols = slice(i * part_dn, (i + 1) * part_dn)
            got = swap(w_down[:, cols], NEAR)
            downs.append((w_down[:, cols], wd_sib[:, cols], got, swap(got, SIB)))

        def up(h2, weights, bias):
            acc = jnp.einsum("bsd,df->bsf", h2, weights, preferred_element_type=F32) + bias.astype(F32)
            return jax.nn.gelu(acc, approximate=True).astype(BF16)

        def up_all(h2):
            return (
                up(h2, *ups[0]),
                up(h2, *ups[1]),
                jnp.concatenate([up(h2, *w) for w in near_parts], axis=-1),
                jnp.concatenate([up(h2, *w) for w in near_sib_parts], axis=-1),
            )

        def down(us, ws):
            return sum(jnp.einsum("bsf,fd->bsd", u, w, preferred_element_type=F32) for u, w in zip(us, ws))

        u_far = [up_all(swap(h2_own, FAR)), up_all(swap(h2_oth, FAR))]
        u_loc = [up_all(h2_own), up_all(h2_oth)]
        outs = [[], []]
        for i in range(n_parts):
            cols = slice(i * part_dn, (i + 1) * part_dn)
            for g, x1 in enumerate((x1_own, x1_oth)):
                back = swap(down(u_far[g], downs[i]).astype(BF16), FAR)
                total = down(u_loc[g], downs[i]) + back.astype(F32)
                outs[g].append((x1[..., cols].astype(F32) + (total + b_down[cols].astype(F32))).astype(BF16))
        first, second = (jnp.concatenate(parts, axis=-1) for parts in outs)
        out = jnp.concatenate([first, second], axis=0)
        return lax.dynamic_update_slice_in_dim(
            lax.dynamic_update_slice_in_dim(out, first, side * half, 0), second, (1 - side) * half, 0
        )

    in_layout = (P("dp", "tp", None), P(), P(), P(None, None, "tp", None), P(None, "tp", None), P("tp", None, None), P(), P(), P(), P(None, "tp"), P("tp"), P("tp", None), P())
    return jax.shard_map(device_body, mesh=mesh, in_specs=in_layout, out_specs=P("dp", "tp", None), check_vma=False)
```
